32 devices in a mesh: row: 8 (over z, x), col: 4 (over y, core).
Axes of the slice: x: 2, y: 2, z: 4, core: 2. Of those that a mesh axis runs over, the one named last changes fastest.
Arguments:
- tiles: bfloat16 [8, 4, 3, 256, 256], P('row', 'col'), as said below
- stack_index: int32 [8, 4, 3], P('row', 'col'), may hold values from 0 to 127, as said below
- block_mask: int32 [64, 64], replicated, may hold values from 0 to 1, as said below
Outputs:
- purified: bfloat16 [8, 4, 3, 256, 256], P('row', 'col')
The draws below stay inside these ranges and needn't reach their ends.
Inputs may be any that keep to these rules, and one draw needn't show every extreme that they name: `block_mask`: the region of one device (8 x 16 blocks) holds at most 3 occupied blocks; some region holds exactly 3 in every draw. `stack_index`: block (a, b) of a device's region is numbered a * 16 + b. A device's 3 entries are distinct and include every occupied block of its region; a slot naming an unoccupied block holds a tile that P does not use. `tiles`: A slot's tile is P's block named by stack_index when that block is occupied.
All inputs are finite; a program needn't handle non-finite values.
Results may differ from the reference program's by a relative error of at most 0.0051.
Values may be sent and summed in bfloat16 or wider, within the bound.
A program may use at most 64 MiB of HBM per device.

```python
import jax
import jax.numpy as jnp
from jax import lax

NB = 64
BS = 256
SLOTS = 3
BR = 8
BC = 16
N_ROW = 8
N_COL = 4


def to_regions(table):
    return table.reshape(N_ROW, BR, N_COL, BC).transpose(0, 2, 1, 3).reshape(N_ROW, N_COL, BR * BC)


def block_layout(key):
    cluster_key = jax.random.fold_in(key, 301)
    anchor_row_key = jax.random.fold_in(key, 302)
    anchor_col_key = jax.random.fold_in(key, 303)
    noise_key = jax.random.fold_in(key, 304)
    mixing_key = jax.random.fold_in(key, 305)
    cluster = jax.random.randint(cluster_key, (NB,), 0, max(NB // 8, 1), dtype=jnp.int32)
    row_iota = jnp.arange(NB, dtype=jnp.int32)[:, None]
    col_iota = jnp.arange(NB, dtype=jnp.int32)[None, :]
    anchor_row = jax.random.randint(anchor_row_key, (), 0, N_ROW, dtype=jnp.int32)
    anchor_col = jax.random.randint(anchor_col_key, (), 0, N_COL, dtype=jnp.int32)
    favoured = (row_iota // BR == anchor_row) & (col_iota // BC == anchor_col)
    candidate = ((cluster[:, None] == cluster[None, :]) | favoured).astype(jnp.int32)
    noise_draw = jax.random.randint(noise_key, (NB, NB), 0, 1024, dtype=jnp.int32)
    priority = candidate * 4096 + noise_draw
    local_count = BR * BC
    local_iota = jnp.arange(local_count, dtype=jnp.int32)
    region_priority = to_regions(priority) * local_count + local_iota
    _, picked = lax.top_k(region_priority, SLOTS)
    picked = picked.astype(jnp.int32)
    kept_slot = jnp.sum((picked[:, :, :, None] == local_iota[None, None, None, :]).astype(jnp.int32), axis=2)
    region_mask = to_regions(candidate) * kept_slot
    occupied = region_mask.reshape(N_ROW, N_COL, BR, BC).transpose(0, 2, 1, 3).reshape(NB, NB)
    mixing = jax.random.randint(mixing_key, (N_ROW, N_COL, SLOTS), 0, 4096, dtype=jnp.int32) * SLOTS + jnp.arange(SLOTS, dtype=jnp.int32)
    placement = jnp.argsort(mixing, axis=2)
    stack_ids = jnp.take_along_axis(picked, placement, axis=2)
    return (occupied, stack_ids)


def draw_block_mask(key, part):
    return block_layout(key)[0]


def draw_stack_index(key, part):
    return block_layout(key)[1]


def draw_tiles(key, part):
    occupied, stack_ids = block_layout(key)
    noise_key = jax.random.fold_in(key, 201)
    tile_shape = (N_ROW, N_COL, SLOTS, BS, BS)
    spread = 1.0 / BS ** 0.5
    noise_draw = spread * jax.random.normal(noise_key, tile_shape, jnp.float32)
    band_row = jnp.arange(N_ROW, dtype=jnp.int32)[:, None, None]
    band_col = jnp.arange(N_COL, dtype=jnp.int32)[None, :, None]
    on_diagonal = band_row * BR + stack_ids // BC == band_col * BC + stack_ids % BC
    identity = jnp.eye(BS, dtype=jnp.float32)
    values = noise_draw + 0.5 * on_diagonal.astype(jnp.float32)[:, :, :, None, None] * identity
    return values.astype(jnp.bfloat16)


def setup_inputs(seed: int = 0) -> dict:
    key_of = jax.random.split(jax.random.key(seed), 4)
    return {
        "tiles": draw_tiles(jax.random.fold_in(key_of[3], 71), 0),
        "stack_index": draw_stack_index(jax.random.fold_in(key_of[3], 71), 0),
        "block_mask": draw_block_mask(jax.random.fold_in(key_of[3], 71), 0),
    }


def reference(tiles, stack_index, block_mask):
    total_slots = N_ROW * N_COL * SLOTS
    flat_tiles = tiles.reshape(total_slots, BS, BS)
    places = jnp.arange(total_slots, dtype=jnp.int32)
    device_id = places // SLOTS
    device_row = device_id // N_COL
    device_col = device_id % N_COL
    flat_ids = stack_index.reshape(total_slots).astype(jnp.int32)
    global_row = (device_row * BR + flat_ids // BC).astype(jnp.int32)
    global_col = (device_col * BC + flat_ids % BC).astype(jnp.int32)
    valid = block_mask[global_row, global_col] > 0
    slot_of = jnp.zeros((NB, NB), jnp.int32).at[global_row, global_col].set(places)

    def product(left_flat, right_flat):
        def per_slot(columns):
            block_row, block_col, live = columns

            def compute(unused):
                def inner(inner_block, total):
                    weight = block_mask[block_row, inner_block] * block_mask[inner_block, block_col]

                    def add_term(running):
                        left_tile = left_flat[slot_of[block_row, inner_block]]
                        right_tile = right_flat[slot_of[inner_block, block_col]]
                        return running + jnp.dot(left_tile, right_tile, preferred_element_type=jnp.float32)

                    def keep_term(running):
                        return running

                    return lax.cond(weight > 0, add_term, keep_term, total)

                return lax.fori_loop(0, NB, inner, jnp.zeros((BS, BS), jnp.float32))

            def skipped(unused):
                return jnp.zeros((BS, BS), jnp.float32)

            return lax.cond(live, compute, skipped, 0)

        return lax.map(per_slot, (global_row, global_col, valid))

    square = product(flat_tiles, flat_tiles).astype(jnp.bfloat16)
    cube_sum = product(square, flat_tiles)
    valid_float = valid.astype(jnp.float32)
    purified = (3.0 * square.astype(jnp.float32) - 2.0 * cube_sum) * valid_float[:, None, None]
    return purified.astype(jnp.bfloat16).reshape(N_ROW, N_COL, SLOTS, BS, BS)
```

```python
import functools

import jax
import jax.numpy as jnp
from jax import lax
from jax.experimental import pallas as pl
from jax.experimental.pallas import tpu as pltpu
from jax.sharding import PartitionSpec as P

MESH = pl.DeviceIdType.MESH
VMEM = pl.BlockSpec(memory_space=pltpu.VMEM)
SMEM = pl.BlockSpec(memory_space=pltpu.SMEM)


def send(src, dst, send_sem, recv_sem, row, col):
    return pltpu.make_async_remote_copy(
        src_ref=src,
        dst_ref=dst,
        send_sem=send_sem,
        recv_sem=recv_sem,
        device_id=(row, col),
        device_id_type=MESH,
    )


def greet(row_size, col_size, row, col, with_rows):
    barrier = pltpu.get_barrier_semaphore()
    count = col_size - 1
    for step in range(1, col_size):
        peer = lax.rem(col + step, col_size)
        pl.semaphore_signal(barrier, inc=1, device_id=(row, peer), device_id_type=MESH)
    if with_rows:
        count += row_size - 1
        for step in range(1, row_size):
            peer = lax.rem(row + step, row_size)
            pl.semaphore_signal(barrier, inc=1, device_id=(peer, col), device_id_type=MESH)
    pl.semaphore_wait(barrier, count)


class ColGather:
    def __init__(self, row, col, col_size, slots, own, panel, sems):
        self.row, self.col, self.slots = row, col, slots
        self.own, self.panel, self.sems = own, panel, sems
        self.chips = col_size // 2
        self.chip, self.core = col // 2, lax.rem(col, 2)
        self.partner = col + 1 - 2 * self.core

    def across(self, step, slot):
        target = 2 * lax.rem(self.chip + step, self.chips) + self.core
        return send(
            self.own.at[slot], self.panel.at[self.col, slot],
            self.sems.at[0, step - 1, slot], self.sems.at[1, step - 1, slot], self.row, target,
        )

    def beside(self, step, slot):
        origin = 2 * lax.rem(self.chip + self.chips - step, self.chips) + self.core
        src = self.own.at[slot] if step == 0 else self.panel.at[origin, slot]
        return send(
            src, self.panel.at[origin, slot],
            self.sems.at[2, step, slot], self.sems.at[3, step, slot], self.row, self.partner,
        )

    def start(self):
        for slot in range(self.slots):
            for step in range(1, self.chips):
                self.across(step, slot).start()
        for slot in range(self.slots):
            self.beside(0, slot).start()

    def forward(self):
        for slot in range(self.slots):
            for step in range(1, self.chips):
                self.across(step, slot).wait_recv()
                self.beside(step, slot).start()

    def finish(self):
        for step in range(self.chips):
            for slot in range(self.slots):
                if step:
                    self.across(step, slot).wait_send()
                self.beside(step, slot).wait()


def gather_kernel(
    row_size, col_size, tiles, ids, left, right, left_ids, right_ids,
    ids_out, col_sems, line_sems, side_sems, row_id_sems, col_id_sems,
):
    row, col = lax.axis_index("row"), lax.axis_index("col")
    slots, side = tiles.shape[0], tiles.shape[1]
    half = side // 2
    length = row_size // 2
    place, lane = row // 2, lax.rem(row, 2)
    mate = row + 1 - 2 * lane

    lane_iota = lax.broadcasted_iota(jnp.int32, (8, 128), 1)
    packed = jnp.full((8, 128), -1, jnp.int32)
    for slot in range(slots):
        packed = jnp.where(lane_iota == slot, ids[0, slot], packed)
    ids_out[...] = packed
    greet(row_size, col_size, row, col, True)

    pieces = [(slot, 0, side, False) for slot in range(slots - 1)]
    pieces += [(slots - 1, half, half, False)]
    early = (slots - 1, 0, half, True)
    mine = [early] + pieces
    count = len(mine)

    def view(ref, piece, origin=None):
        slot, first, rows, _ = piece
        if origin is None:
            return ref.at[slot, pl.ds(first, rows)]
        return ref.at[origin, slot, pl.ds(first, rows)]

    def to_mate(index, at):
        piece = mine[index]
        origin = 2 * at + lane
        return send(
            view(right, piece, origin), view(right, piece, origin),
            side_sems.at[0, at, index], side_sems.at[1, at, index], mate, col,
        )

    def own_to_mate(index):
        piece = mine[index]
        return send(
            view(tiles, piece), view(right, piece, row),
            side_sems.at[0, place, index], side_sems.at[1, place, index], mate, col,
        )

    def from_mate(index, at):
        piece = mine[index]
        origin = 2 * at + 1 - lane
        return send(
            view(right, piece, origin), view(right, piece, origin),
            side_sems.at[0, at, index], side_sems.at[1, at, index], mate, col,
        )

    def along(way, step, index, first=False):
        heading = 1 if way == 0 else -1
        piece = mine[0] if index == count else mine[index]
        on_lane = 1 - lane if index == count else lane
        origin = 2 * (place - heading * step) + on_lane
        src = view(tiles, piece) if first and index < count else view(right, piece, origin)
        return send(
            src, view(right, piece, origin),
            line_sems.at[way, 0, step, index], line_sems.at[way, 1, step, index],
            row + 2 * heading, col,
        )

    def landing(way, step, index):
        heading = 1 if way == 0 else -1
        piece = mine[0] if index == count else mine[index]
        on_lane = 1 - lane if index == count else lane
        origin = 2 * (place - heading * (step + 1)) + on_lane
        return send(
            view(right, piece, origin), view(right, piece, origin),
            line_sems.at[way, 0, step, index], line_sems.at[way, 1, step, index],
            row + 2 * heading, col,
        )

    can_send = (place + 1 < length, place > 0)

    def arrives(way, step):
        return place - step >= 1 if way == 0 else place + step + 1 < length

    def goes(way, step):
        if way == 0:
            return (place - step >= 0) & (place + 1 < length)
        return (place + step < length) & (place > 0)

    own_to_mate(0).start()
    for index in range(count):
        for way in range(2):
            @pl.when(can_send[way])
            def _():
                along(way, 0, index, True).start()
        if index:
            own_to_mate(index).start()
    left_gather = ColGather(row, col, col_size, slots, tiles, left, col_sems)
    left_gather.start()

    def id_row(step):
        return send(
            ids_out, right_ids.at[row], row_id_sems.at[0, step], row_id_sems.at[1, step],
            lax.rem(row + step, row_size), col,
        )

    def id_col(step):
        return send(
            ids_out, left_ids.at[col], col_id_sems.at[0, step], col_id_sems.at[1, step],
            row, lax.rem(col + step, col_size),
        )

    for step in range(1, row_size):
        id_row(step).start()
    for step in range(1, col_size):
        id_col(step).start()

    from_mate(0, place).wait_recv()
    for way in range(2):
        @pl.when(can_send[way])
        def _():
            along(way, 0, count).start()

    right[row] = tiles[...]
    left[col] = tiles[...]
    right_ids[row] = packed
    left_ids[col] = packed

    def turn(step, unused):
        for index in list(range(count)) + [count]:
            for way in range(2):
                @pl.when(arrives(way, step))
                def _():
                    landing(way, step, index).wait_recv()

                    @pl.when(can_send[way])
                    def _():
                        along(way, step + 1, index).start()

                    if 0 < index < count:
                        heading = 1 if way == 0 else -1
                        to_mate(index, place - heading * (step + 1)).start()
        return unused

    turn(0, 0)
    left_gather.forward()
    lax.fori_loop(1, length - 1, turn, 0)

    left_gather.finish()
    for step in range(1, row_size):
        id_row(step).wait()
    for step in range(1, col_size):
        id_col(step).wait()

    def settle(step, unused):
        for index in range(count + 1):
            for way in range(2):
                @pl.when(goes(way, step))
                def _():
                    along(way, step, index).wait_send()
        return unused

    lax.fori_loop(0, length - 1, settle, 0)
    own_to_mate(0).wait_send()

    def collect(at, unused):
        for index in range(1, count):
            to_mate(index, at).wait_send()
            from_mate(index, at).wait_recv()
        return unused

    lax.fori_loop(0, length, collect, 0)


def squares_kernel(row_size, col_size, square, panel, col_sems):
    row, col = lax.axis_index("row"), lax.axis_index("col")
    greet(row_size, col_size, row, col, False)
    gather = ColGather(row, col, col_size, square.shape[0], square, panel, col_sems)
    gather.start()
    panel[col] = square[...]
    gather.forward()
    gather.finish()


def products(row_size, col_size, left, right, left_ids, right_ids, mask, total):
    row, col = lax.axis_index("row"), lax.axis_index("col")
    slots = total.shape[0]
    block_rows, block_cols = mask.shape[0] // row_size, mask.shape[1] // col_size
    total[...] = jnp.zeros_like(total)
    for slot in range(slots):
        own = left_ids[col, 0, slot]
        own_row = own // block_cols
        out_row = row * block_rows + own_row
        out_col = col * block_cols + lax.rem(own, block_cols)
        live = mask[out_row, out_col] > 0

        @pl.when(live)
        def _():
            def panel_step(region, unused):
                for place in range(slots):
                    label = left_ids[region, 0, place]
                    inner = region * block_cols + lax.rem(label, block_cols)
                    use = (label // block_cols == own_row) & (mask[out_row, inner] > 0)
                    use = use & (mask[inner, out_col] > 0)

                    @pl.when(use)
                    def _():
                        band = inner // block_rows
                        wanted = lax.rem(inner, block_rows) * block_cols + lax.rem(own, block_cols)
                        spot = jnp.int32(0)
                        for other in range(1, slots):
                            spot = jnp.where(right_ids[band, 0, other] == wanted, other, spot)
                        total[slot] += jnp.dot(
                            left[region, place], right[band, spot], preferred_element_type=jnp.float32
                        )
                return unused

            lax.fori_loop(0, col_size, panel_step, 0)


def square_kernel(row_size, col_size, left, right, left_ids, right_ids, mask, out, total):
    products(row_size, col_size, left, right, left_ids, right_ids, mask, total)
    out[...] = total[...].astype(out.dtype)


def cube_kernel(row_size, col_size, square, right, left_ids, right_ids, mask, out, total):
    products(row_size, col_size, square, right, left_ids, right_ids, mask, total)
    col = lax.axis_index("col")
    out[...] = (3.0 * square[col].astype(jnp.float32) - 2.0 * total[...]).astype(out.dtype)


def solution(mesh):
    row_size, col_size = mesh.shape["row"], mesh.shape["col"]
    length, chips = row_size // 2, col_size // 2
    dma = pltpu.SemaphoreType.DMA

    def local(tiles, stack_index, block_mask):
        stack, ids = tiles[0, 0], stack_index[0]
        slots, side, _ = stack.shape
        shape = jax.ShapeDtypeStruct
        col_sems = dma((4, chips, slots))
        left, right, left_ids, right_ids = pl.pallas_call(
            functools.partial(gather_kernel, row_size, col_size),
            out_shape=(
                shape((col_size, slots, side, side), stack.dtype),
                shape((row_size, slots, side, side), stack.dtype),
                shape((col_size, 8, 128), jnp.int32),
                shape((row_size, 8, 128), jnp.int32),
            ),
            in_specs=[VMEM, SMEM],
            out_specs=(VMEM,) * 4,
            scratch_shapes=[
                pltpu.VMEM((8, 128), jnp.int32),
                col_sems,
                dma((2, 2, length, slots + 2)),
                dma((2, length, slots + 1)),
                dma((2, row_size)),
                dma((2, col_size)),
            ],
            compiler_params=pltpu.CompilerParams(collective_id=0, has_side_effects=True),
            name="gather",
        )(stack, ids)
        square = pl.pallas_call(
            functools.partial(square_kernel, row_size, col_size),
            out_shape=shape(stack.shape, stack.dtype),
            in_specs=[VMEM, VMEM, SMEM, SMEM, SMEM],
            out_specs=VMEM,
            scratch_shapes=[pltpu.VMEM(stack.shape, jnp.float32)],
            name="square",
        )(left, right, left_ids, right_ids, block_mask)
        squares = pl.pallas_call(
            functools.partial(squares_kernel, row_size, col_size),
            out_shape=shape((col_size, slots, side, side), stack.dtype),
            in_specs=[VMEM],
            out_specs=VMEM,
            scratch_shapes=[col_sems],
            compiler_params=pltpu.CompilerParams(collective_id=1, has_side_effects=True),
            name="squares",
        )(square)
        purified = pl.pallas_call(
            functools.partial(cube_kernel, row_size, col_size),
            out_shape=shape(stack.shape, stack.dtype),
            in_specs=[VMEM, VMEM, SMEM, SMEM, SMEM],
            out_specs=VMEM,
            scratch_shapes=[pltpu.VMEM(stack.shape, jnp.float32)],
            name="cube",
        )(squares, right, left_ids, right_ids, block_mask)
        return purified[None, None]

    placed = (P("row", "col", None, None, None), P("row", "col", None), P())
    return jax.shard_map(
        local,
        mesh=mesh,
        in_specs=placed,
        out_specs=P("row", "col", None, None, None),
        check_vma=False,
    )
```

```python
import functools

import jax
import jax.numpy as jnp
from jax import lax
from jax.experimental import pallas as pl
from jax.experimental.pallas import tpu as pltpu
from jax.sharding import PartitionSpec as P

MESH = pl.DeviceIdType.MESH
VMEM = pl.BlockSpec(memory_space=pltpu.VMEM)
SMEM = pl.BlockSpec(memory_space=pltpu.SMEM)


def send(src, dst, send_sem, recv_sem, row, col):
    return pltpu.make_async_remote_copy(
        src_ref=src,
        dst_ref=dst,
        send_sem=send_sem,
        recv_sem=recv_sem,
        device_id=(row, col),
        device_id_type=MESH,
    )


def greet(row_size, col_size, row, col, with_rows):
    barrier = pltpu.get_barrier_semaphore()
    count = col_size - 1
    for step in range(1, col_size):
        peer = lax.rem(col + step, col_size)
        pl.semaphore_signal(barrier, inc=1, device_id=(row, peer), device_id_type=MESH)
    if with_rows:
        count += row_size - 1
        for step in range(1, row_size):
            peer = lax.rem(row + step, row_size)
            pl.semaphore_signal(barrier, inc=1, device_id=(peer, col), device_id_type=MESH)
    pl.semaphore_wait(barrier, count)


class ColGather:
    def __init__(self, row, col, col_size, slots, own, panel, sems):
        self.row, self.col, self.slots = row, col, slots
        self.own, self.panel, self.sems = own, panel, sems
        self.chips = col_size // 2
        self.chip, self.core = col // 2, lax.rem(col, 2)
        self.partner = col + 1 - 2 * self.core

    def across(self, step, slot):
        target = 2 * lax.rem(self.chip + step, self.chips) + self.core
        return send(
            self.own.at[slot], self.panel.at[self.col, slot],
            self.sems.at[0, step - 1, slot], self.sems.at[1, step - 1, slot], self.row, target,
        )

    def beside(self, step, slot):
        origin = 2 * lax.rem(self.chip + self.chips - step, self.chips) + self.core
        src = self.own.at[slot] if step == 0 else self.panel.at[origin, slot]
        return send(
            src, self.panel.at[origin, slot],
            self.sems.at[2, step, slot], self.sems.at[3, step, slot], self.row, self.partner,
        )

    def start(self):
        for slot in range(self.slots):
            for step in range(1, self.chips):
                self.across(step, slot).start()
        for slot in range(self.slots):
            self.beside(0, slot).start()

    def origin(self, step, core):
        return 2 * lax.rem(self.chip + self.chips - step, self.chips) + core

    def forward(self, use=None):
        for slot in range(self.slots):
            for step in range(1, self.chips):
                self.across(step, slot).wait_recv()
                self.beside(step, slot).start()
                if use is not None:
                    use(self.origin(step, self.core), slot)

    def collect(self, use, steps):
        for step in steps:
            for slot in range(self.slots):
                self.beside(step, slot).wait_recv()
                if use is not None:
                    use(self.origin(step, 1 - self.core), slot)

    def settle(self):
        for step in range(self.chips):
            for slot in range(self.slots):
                if step:
                    self.across(step, slot).wait_send()
                self.beside(step, slot).wait_send()


def kernel(
    row_size, col_size, tiles, ids, mask, out, left, right, squares, square, total, left_ids, right_ids, ids_out,
    left_labels, right_labels, col_sems, square_sems, line_sems, side_sems, row_id_sems, col_id_sems, label_sems,
):
    row, col = lax.axis_index("row"), lax.axis_index("col")
    slots, side = tiles.shape[0], tiles.shape[1]
    half = side // 2
    length = row_size // 2
    place, lane = row // 2, lax.rem(row, 2)
    mate = row + 1 - 2 * lane

    lane_iota = lax.broadcasted_iota(jnp.int32, (8, 128), 1)
    packed = jnp.full((8, 128), -1, jnp.int32)
    for slot in range(slots):
        packed = jnp.where(lane_iota == slot, ids[0, slot], packed)
    ids_out[...] = packed
    greet(row_size, col_size, row, col, True)

    pieces = [(slot, 0, side, False) for slot in range(slots - 1)]
    pieces += [(slots - 1, half, half, False)]
    early = (slots - 1, 0, half, True)
    mine = [early] + pieces
    count = len(mine)

    def view(ref, piece, origin=None):
        slot, first, rows, _ = piece
        if origin is None:
            return ref.at[slot, pl.ds(first, rows)]
        return ref.at[origin, slot, pl.ds(first, rows)]

    def to_mate(index, at):
        piece = mine[index]
        origin = 2 * at + lane
        return send(
            view(right, piece, origin), view(right, piece, origin),
            side_sems.at[0, at, index], side_sems.at[1, at, index], mate, col,
        )

    def own_to_mate(index):
        piece = mine[index]
        return send(
            view(tiles, piece), view(right, piece, row),
            side_sems.at[0, place, index], side_sems.at[1, place, index], mate, col,
        )

    def from_mate(index, at):
        piece = mine[index]
        origin = 2 * at + 1 - lane
        return send(
            view(right, piece, origin), view(right, piece, origin),
            side_sems.at[0, at, index], side_sems.at[1, at, index], mate, col,
        )

    def along(way, step, index, first=False):
        heading = 1 if way == 0 else -1
        piece = mine[0] if index == count else mine[index]
        on_lane = 1 - lane if index == count else lane
        origin = 2 * (place - heading * step) + on_lane
        src = view(tiles, piece) if first and index < count else view(right, piece, origin)
        return send(
            src, view(right, piece, origin),
            line_sems.at[way, 0, step, index], line_sems.at[way, 1, step, index],
            row + 2 * heading, col,
        )

    def landing(way, step, index):
        heading = 1 if way == 0 else -1
        piece = mine[0] if index == count else mine[index]
        on_lane = 1 - lane if index == count else lane
        origin = 2 * (place - heading * (step + 1)) + on_lane
        return send(
            view(right, piece, origin), view(right, piece, origin),
            line_sems.at[way, 0, step, index], line_sems.at[way, 1, step, index],
            row + 2 * heading, col,
        )

    can_send = (place + 1 < length, place > 0)

    def arrives(way, step):
        return place - step >= 1 if way == 0 else place + step + 1 < length

    def goes(way, step):
        if way == 0:
            return (place - step >= 0) & (place + 1 < length)
        return (place + step < length) & (place > 0)

    own_to_mate(0).start()
    for index in range(count):
        for way in range(2):
            @pl.when(can_send[way])
            def _():
                along(way, 0, index, True).start()
        if index:
            own_to_mate(index).start()
    left_gather = ColGather(row, col, col_size, slots, tiles, left, col_sems)
    left_gather.start()

    def id_row(step):
        return send(
            ids_out, right_ids.at[row], row_id_sems.at[0, step], row_id_sems.at[1, step],
            lax.rem(row + step, row_size), col,
        )

    def id_col(step):
        return send(
            ids_out, left_ids.at[col], col_id_sems.at[0, step], col_id_sems.at[1, step],
            row, lax.rem(col + step, col_size),
        )

    for step in range(1, row_size):
        id_row(step).start()
    for step in range(1, col_size):
        id_col(step).start()

    from_mate(0, place).wait_recv()
    for way in range(2):
        @pl.when(can_send[way])
        def _():
            along(way, 0, count).start()

    right[row] = tiles[...]
    left[col] = tiles[...]
    right_ids[row] = packed
    left_ids[col] = packed

    def turn(step, unused):
        for index in list(range(count)) + [count]:
            for way in range(2):
                @pl.when(arrives(way, step))
                def _():
                    landing(way, step, index).wait_recv()

                    @pl.when(can_send[way])
                    def _():
                        along(way, step + 1, index).start()

                    if 0 < index < count:
                        heading = 1 if way == 0 else -1
                        to_mate(index, place - heading * (step + 1)).start()
        return unused

    block_rows, block_cols = mask.shape[0] // row_size, mask.shape[1] // col_size
    owns = []
    for slot in range(slots):
        own = ids[0, slot]
        own_row, own_col = own // block_cols, lax.rem(own, block_cols)
        out_row, out_col = row * block_rows + own_row, col * block_cols + own_col
        owns.append((own_row, own_col, out_row, out_col, mask[out_row, out_col] > 0))

    def find(labels, region, wanted):
        spot, found = jnp.int32(0), labels[region, 0, 0] == wanted
        for other in range(1, slots):
            same = labels[region, 0, other] == wanted
            spot = jnp.where(same, other, spot)
            found = found | same
        return spot, found

    def square_term(origin, place):
        label = right_labels[origin, 0, place]
        inner = origin * block_rows + label // block_cols
        band = inner // block_cols
        chosen = []
        for own_row, own_col, out_row, out_col, live in owns:
            spot, found = find(left_labels, band, own_row * block_cols + lax.rem(inner, block_cols))
            use = live & found & (lax.rem(label, block_cols) == own_col)
            use = use & (mask[out_row, inner] > 0) & (mask[inner, out_col] > 0)
            tile = left[band, spot]
            chosen.append(jnp.where(use, tile, jnp.zeros_like(tile)))
        term = jnp.dot(
            jnp.concatenate(chosen, axis=0), right[origin, place], preferred_element_type=jnp.float32
        )
        total[...] += term.reshape(total.shape)

    def cube_term(origin, place):
        label = left_labels[origin, 0, place]
        inner = origin * block_cols + lax.rem(label, block_cols)
        band = inner // block_rows
        piece = squares[origin, place]
        for slot, (own_row, own_col, out_row, out_col, live) in enumerate(owns):
            spot, found = find(right_labels, band, lax.rem(inner, block_rows) * block_cols + own_col)
            use = live & found & (label // block_cols == own_row)
            use = use & (mask[out_row, inner] > 0) & (mask[inner, out_col] > 0)
            tile = right[band, spot]
            total[slot] += jnp.dot(
                piece, jnp.where(use, tile, jnp.zeros_like(tile)), preferred_element_type=jnp.float32
            )

    def stack_terms(origin, wait=None):
        for slot in range(slots):
            if wait is not None:
                wait(slot)
            square_term(origin, slot)

    def mate_terms(at):
        stack_terms(2 * at + 1 - lane, lambda slot: from_mate(slot + 1, at).wait_recv())

    def consume(step):
        for way in range(2):
            @pl.when(arrives(way, step))
            def _():
                heading = 1 if way == 0 else -1
                stack_terms(2 * (place - heading * (step + 1)) + lane)
        for way in range(2):
            @pl.when(arrives(way, step))
            def _():
                heading = 1 if way == 0 else -1
                mate_terms(place - heading * (step + 1))

    total[...] = jnp.zeros_like(total)
    for step in range(1, row_size):
        id_row(step).wait()
    for step in range(1, col_size):
        id_col(step).wait()
    copies = (
        pltpu.make_async_copy(left_ids, left_labels, label_sems.at[0]),
        pltpu.make_async_copy(right_ids, right_labels, label_sems.at[1]),
    )
    for copy in copies:
        copy.start()
    for copy in copies:
        copy.wait()
    turn(0, 0)
    left_gather.forward()
    left_gather.collect(None, range(left_gather.chips))
    stack_terms(row)
    mate_terms(place)

    def advance(step, unused):
        turn(step, 0)
        consume(step - 1)
        return unused

    lax.fori_loop(1, length - 1, advance, 0)
    consume(length - 2)

    square[...] = total[...].astype(square.dtype)

    def keep(slot, unused):
        squares[col, slot] = square[slot]
        return unused

    lax.fori_loop(0, slots, keep, 0)
    square_gather = ColGather(row, col, col_size, slots, square, squares, square_sems)
    square_gather.start()
    total[...] = jnp.zeros_like(total)
    for slot in range(slots):
        cube_term(col, slot)
    square_gather.collect(cube_term, [0])
    square_gather.forward(cube_term)
    square_gather.collect(cube_term, range(1, square_gather.chips))
    out[...] = (3.0 * square[...].astype(jnp.float32) - 2.0 * total[...]).astype(out.dtype)

    left_gather.settle()
    square_gather.settle()

    def settle(step, unused):
        for index in range(count + 1):
            for way in range(2):
                @pl.when(goes(way, step))
                def _():
                    along(way, step, index).wait_send()
        return unused

    lax.fori_loop(0, length - 1, settle, 0)
    own_to_mate(0).wait_send()

    def collect(at, unused):
        for index in range(1, count):
            to_mate(index, at).wait_send()
        return unused

    lax.fori_loop(0, length, collect, 0)


def solution(mesh):
    row_size, col_size = mesh.shape["row"], mesh.shape["col"]
    length, chips = row_size // 2, col_size // 2
    dma = pltpu.SemaphoreType.DMA

    def local(tiles, stack_index, block_mask):
        stack, ids = tiles[0, 0], stack_index[0]
        slots, side, _ = stack.shape
        col_panel = pltpu.VMEM((col_size, slots, side, side), stack.dtype)
        purified = pl.pallas_call(
            functools.partial(kernel, row_size, col_size),
            out_shape=jax.ShapeDtypeStruct(stack.shape, stack.dtype),
            in_specs=[VMEM, SMEM, SMEM],
            out_specs=VMEM,
            scratch_shapes=[
                col_panel,
                pltpu.VMEM((row_size, slots, side, side), stack.dtype),
                col_panel,
                pltpu.VMEM(stack.shape, stack.dtype),
                pltpu.VMEM(stack.shape, jnp.float32),
                pltpu.VMEM((col_size, 8, 128), jnp.int32),
                pltpu.VMEM((row_size, 8, 128), jnp.int32),
                pltpu.VMEM((8, 128), jnp.int32),
                pltpu.SMEM((col_size, 8, 128), jnp.int32),
                pltpu.SMEM((row_size, 8, 128), jnp.int32),
                dma((4, chips, slots)),
                dma((4, chips, slots)),
                dma((2, 2, length, slots + 2)),
                dma((2, length, slots + 1)),
                dma((2, row_size)),
                dma((2, col_size)),
                dma((2,)),
            ],
            compiler_params=pltpu.CompilerParams(collective_id=0, has_side_effects=True),
            name="purify",
        )(stack, ids, block_mask)
        return purified[None, None]

    placed = (P("row", "col", None, None, None), P("row", "col", None), P())
    return jax.shard_map(
        local,
        mesh=mesh,
        in_specs=placed,
        out_specs=P("row", "col", None, None, None),
        check_vma=False,
    )
```

```python
import functools

import jax
import jax.numpy as jnp
from jax import lax
from jax.experimental import pallas as pl
from jax.experimental.pallas import tpu as pltpu
from jax.sharding import PartitionSpec as P

MESH = pl.DeviceIdType.MESH
VMEM = pl.BlockSpec(memory_space=pltpu.VMEM)
SMEM = pl.BlockSpec(memory_space=pltpu.SMEM)


def send(src, dst, send_sem, recv_sem, row, col):
    return pltpu.make_async_remote_copy(
        src_ref=src,
        dst_ref=dst,
        send_sem=send_sem,
        recv_sem=recv_sem,
        device_id=(row, col),
        device_id_type=MESH,
    )


def greet(row_size, col_size, row, col, with_rows):
    barrier = pltpu.get_barrier_semaphore()
    count = col_size - 1
    for step in range(1, col_size):
        peer = lax.rem(col + step, col_size)
        pl.semaphore_signal(barrier, inc=1, device_id=(row, peer), device_id_type=MESH)
    if with_rows:
        count += row_size - 1
        for step in range(1, row_size):
            peer = lax.rem(row + step, row_size)
            pl.semaphore_signal(barrier, inc=1, device_id=(peer, col), device_id_type=MESH)
    pl.semaphore_wait(barrier, count)


class ColGather:
    def __init__(self, row, col, col_size, slots, own, panel, sems, part, start, width):
        self.columns, self.part = pl.ds(start, width), 4 * part
        self.row, self.col, self.slots = row, col, slots
        self.own, self.panel, self.sems = own, panel, sems
        self.chips = col_size // 2
        self.chip, self.core = col // 2, lax.rem(col, 2)
        self.partner = col + 1 - 2 * self.core

    def across(self, step, slot):
        target = 2 * lax.rem(self.chip + step, self.chips) + self.core
        return send(
            self.own.at[slot, :, self.columns], self.panel.at[self.col, slot, :, self.columns],
            self.sems.at[self.part, step - 1, slot], self.sems.at[self.part + 1, step - 1, slot],
            self.row, target,
        )

    def beside(self, step, slot):
        origin = 2 * lax.rem(self.chip + self.chips - step, self.chips) + self.core
        panel = self.panel.at[origin, slot, :, self.columns]
        src = self.own.at[slot, :, self.columns] if step == 0 else panel
        return send(
            src, panel,
            self.sems.at[self.part + 2, step, slot], self.sems.at[self.part + 3, step, slot],
            self.row, self.partner,
        )

    def start(self):
        for slot in range(self.slots):
            for step in range(1, self.chips):
                self.across(step, slot).start()
        for slot in range(self.slots):
            self.beside(0, slot).start()

    def origin(self, step, core):
        return 2 * lax.rem(self.chip + self.chips - step, self.chips) + core

    def forward(self, use=None):
        for slot in range(self.slots):
            for step in range(1, self.chips):
                self.across(step, slot).wait_recv()
                self.beside(step, slot).start()
                if use is not None:
                    use(self.origin(step, self.core), slot)

    def collect(self, use, steps):
        for step in steps:
            for slot in range(self.slots):
                self.beside(step, slot).wait_recv()
                if use is not None:
                    use(self.origin(step, 1 - self.core), slot)

    def settle(self):
        for step in range(self.chips):
            for slot in range(self.slots):
                if step:
                    self.across(step, slot).wait_send()
                self.beside(step, slot).wait_send()


def kernel(
    row_size, col_size, tiles, ids, mask, out, left, right, squares, square, total, left_ids, right_ids, ids_out,
    left_labels, right_labels, col_sems, square_sems, line_sems, side_sems, row_id_sems, col_id_sems, label_sems,
):
    row, col = lax.axis_index("row"), lax.axis_index("col")
    slots, side = tiles.shape[0], tiles.shape[1]
    half = side // 2
    length = row_size // 2
    place, lane = row // 2, lax.rem(row, 2)
    mate = row + 1 - 2 * lane

    lane_iota = lax.broadcasted_iota(jnp.int32, (8, 128), 1)
    packed = jnp.full((8, 128), -1, jnp.int32)
    for slot in range(slots):
        packed = jnp.where(lane_iota == slot, ids[0, slot], packed)
    ids_out[...] = packed
    greet(row_size, col_size, row, col, True)

    pieces = [(slot, 0, side, False) for slot in range(slots - 1)]
    pieces += [(slots - 1, half, half, False)]
    early = (slots - 1, 0, half, True)
    mine = [early] + pieces
    count = len(mine)

    def view(ref, piece, part, origin=None):
        slot, first, rows, _ = piece
        columns = pl.ds(part * half, half)
        if origin is None:
            return ref.at[slot, pl.ds(first, rows), columns]
        return ref.at[origin, slot, pl.ds(first, rows), columns]

    def to_mate(index, at, part):
        piece = mine[index]
        origin = 2 * at + lane
        return send(
            view(right, piece, part, origin), view(right, piece, part, origin),
            side_sems.at[2 * part, at, index], side_sems.at[2 * part + 1, at, index], mate, col,
        )

    def own_to_mate(index, part):
        piece = mine[index]
        return send(
            view(tiles, piece, part), view(right, piece, part, row),
            side_sems.at[2 * part, place, index], side_sems.at[2 * part + 1, place, index], mate, col,
        )

    def from_mate(index, at, part):
        piece = mine[index]
        origin = 2 * at + 1 - lane
        return send(
            view(right, piece, part, origin), view(right, piece, part, origin),
            side_sems.at[2 * part, at, index], side_sems.at[2 * part + 1, at, index], mate, col,
        )

    def along(way, step, index, part, first=False):
        heading = 1 if way == 0 else -1
        piece = mine[0] if index == count else mine[index]
        on_lane = 1 - lane if index == count else lane
        origin = 2 * (place - heading * step) + on_lane
        src = view(tiles, piece, part) if first and index < count else view(right, piece, part, origin)
        return send(
            src, view(right, piece, part, origin),
            line_sems.at[2 * part + way, 0, step, index], line_sems.at[2 * part + way, 1, step, index],
            row + 2 * heading, col,
        )

    def landing(way, step, index, part):
        heading = 1 if way == 0 else -1
        piece = mine[0] if index == count else mine[index]
        on_lane = 1 - lane if index == count else lane
        origin = 2 * (place - heading * (step + 1)) + on_lane
        return send(
            view(right, piece, part, origin), view(right, piece, part, origin),
            line_sems.at[2 * part + way, 0, step, index], line_sems.at[2 * part + way, 1, step, index],
            row + 2 * heading, col,
        )

    can_send = (place + 1 < length, place > 0)

    def arrives(way, step):
        return place - step >= 1 if way == 0 else place + step + 1 < length

    def goes(way, step):
        if way == 0:
            return (place - step >= 0) & (place + 1 < length)
        return (place + step < length) & (place > 0)

    def begin(part):
        own_to_mate(0, part).start()
        for index in range(count):
            for way in range(2):
                @pl.when(can_send[way])
                def _():
                    along(way, 0, index, part, True).start()
            if index:
                own_to_mate(index, part).start()

    def begin_mate(part):
        from_mate(0, place, part).wait_recv()
        for way in range(2):
            @pl.when(can_send[way])
            def _():
                along(way, 0, count, part).start()

    begin(0)
    left_gather = ColGather(row, col, col_size, slots, tiles, left, col_sems, 0, 0, side)
    left_gather.start()

    def id_row(step):
        return send(
            ids_out, right_ids.at[row], row_id_sems.at[0, step], row_id_sems.at[1, step],
            lax.rem(row + step, row_size), col,
        )

    def id_col(step):
        return send(
            ids_out, left_ids.at[col], col_id_sems.at[0, step], col_id_sems.at[1, step],
            row, lax.rem(col + step, col_size),
        )

    for step in range(1, row_size):
        id_row(step).start()
    for step in range(1, col_size):
        id_col(step).start()

    begin_mate(0)

    right[row] = tiles[...]
    left[col] = tiles[...]
    right_ids[row] = packed
    left_ids[col] = packed

    def turn(step, part):
        for index in list(range(count)) + [count]:
            for way in range(2):
                @pl.when(arrives(way, step))
                def _():
                    landing(way, step, index, part).wait_recv()

                    @pl.when(can_send[way])
                    def _():
                        along(way, step + 1, index, part).start()

                    if 0 < index < count:
                        heading = 1 if way == 0 else -1
                        to_mate(index, place - heading * (step + 1), part).start()

    block_rows, block_cols = mask.shape[0] // row_size, mask.shape[1] // col_size
    owns = []
    for slot in range(slots):
        own = ids[0, slot]
        own_row, own_col = own // block_cols, lax.rem(own, block_cols)
        out_row, out_col = row * block_rows + own_row, col * block_cols + own_col
        owns.append((own_row, own_col, out_row, out_col, mask[out_row, out_col] > 0))

    def find(labels, region, wanted):
        spot, found = jnp.int32(0), labels[region, 0, 0] == wanted
        for other in range(1, slots):
            same = labels[region, 0, other] == wanted
            spot = jnp.where(same, other, spot)
            found = found | same
        return spot, found

    def square_term(origin, place, part):
        label = right_labels[origin, 0, place]
        inner = origin * block_rows + label // block_cols
        band = inner // block_cols
        chosen = []
        for own_row, own_col, out_row, out_col, live in owns:
            spot, found = find(left_labels, band, own_row * block_cols + lax.rem(inner, block_cols))
            use = live & found & (lax.rem(label, block_cols) == own_col)
            use = use & (mask[out_row, inner] > 0) & (mask[inner, out_col] > 0)
            tile = left[band, spot]
            chosen.append(jnp.where(use, tile, jnp.zeros_like(tile)))
        term = jnp.dot(
            jnp.concatenate(chosen, axis=0),
            right[origin, place, :, part * half:(part + 1) * half],
            preferred_element_type=jnp.float32,
        )
        total[:, :, part * half:(part + 1) * half] += term.reshape(slots, side, half)

    def cube_term(origin, place, part):
        label = left_labels[origin, 0, place]
        inner = origin * block_cols + lax.rem(label, block_cols)
        band = inner // block_rows
        piece = squares[origin, place, :, part * half:(part + 1) * half]
        for slot, (own_row, own_col, out_row, out_col, live) in enumerate(owns):
            spot, found = find(right_labels, band, lax.rem(inner, block_rows) * block_cols + own_col)
            use = live & found & (label // block_cols == own_row)
            use = use & (mask[out_row, inner] > 0) & (mask[inner, out_col] > 0)
            tile = right[band, spot, part * half:(part + 1) * half, :]
            total[slot] += jnp.dot(
                piece, jnp.where(use, tile, jnp.zeros_like(tile)), preferred_element_type=jnp.float32
            )

    def stack_terms(origin, part, wait=None):
        for slot in range(slots):
            if wait is not None:
                wait(slot)
            square_term(origin, slot, part)

    def mate_terms(at, part):
        stack_terms(2 * at + 1 - lane, part, lambda slot: from_mate(slot + 1, at, part).wait_recv())

    def consume(step, part):
        for way in range(2):
            @pl.when(arrives(way, step))
            def _():
                heading = 1 if way == 0 else -1
                stack_terms(2 * (place - heading * (step + 1)) + lane, part)
        for way in range(2):
            @pl.when(arrives(way, step))
            def _():
                heading = 1 if way == 0 else -1
                mate_terms(place - heading * (step + 1), part)

    def over(first, last, *bodies):
        def body(step, unused):
            for each in bodies:
                each(step)
            return unused

        lax.fori_loop(first, last, body, 0)

    def finish(part):
        columns = slice(part * half, (part + 1) * half)
        square[:, :, columns] = total[:, :, columns].astype(square.dtype)

        def keep(slot):
            squares[col, slot, :, columns] = square[slot, :, columns]

        over(0, slots, keep)
        gather = ColGather(
            row, col, col_size, slots, square, squares, square_sems, part, part * half, half
        )
        gather.start()
        return gather

    total[...] = jnp.zeros_like(total)
    for step in range(1, row_size):
        id_row(step).wait()
    for step in range(1, col_size):
        id_col(step).wait()
    copies = (
        pltpu.make_async_copy(left_ids, left_labels, label_sems.at[0]),
        pltpu.make_async_copy(right_ids, right_labels, label_sems.at[1]),
    )
    for copy in copies:
        copy.start()
    for copy in copies:
        copy.wait()
    second = min(2, length - 1)
    for step in range(second):
        turn(step, 0)
    left_gather.forward()
    left_gather.collect(None, range(left_gather.chips))
    stack_terms(row, 0)
    mate_terms(place, 0)
    over(second, length - 1, lambda step: turn(step, 0))
    begin(1)
    begin_mate(1)
    over(0, length - 2, lambda step: consume(step, 0))
    turn(0, 1)
    consume(length - 2, 0)
    first_gather = finish(0)
    stack_terms(row, 1)
    mate_terms(place, 1)
    over(1, length - 1, lambda step: turn(step, 1), lambda step: consume(step - 1, 1))
    first_gather.forward()
    consume(length - 2, 1)
    second_gather = finish(1)

    total[...] = jnp.zeros_like(total)

    def first_term(origin, slot):
        cube_term(origin, slot, 0)

    def second_term(origin, slot):
        cube_term(origin, slot, 1)

    for slot in range(slots):
        first_term(col, slot)
    for step in range(1, first_gather.chips):
        for slot in range(slots):
            first_term(first_gather.origin(step, first_gather.core), slot)
    first_gather.collect(first_term, range(first_gather.chips))
    for slot in range(slots):
        second_term(col, slot)
    second_gather.collect(second_term, [0])
    second_gather.forward(second_term)
    second_gather.collect(second_term, range(1, second_gather.chips))
    out[...] = (3.0 * square[...].astype(jnp.float32) - 2.0 * total[...]).astype(out.dtype)

    left_gather.settle()
    first_gather.settle()
    second_gather.settle()

    def settle(step):
        for part in range(2):
            for index in range(count + 1):
                for way in range(2):
                    @pl.when(goes(way, step))
                    def _():
                        along(way, step, index, part).wait_send()

    def collect(at):
        for part in range(2):
            for index in range(1, count):
                to_mate(index, at, part).wait_send()

    over(0, length - 1, settle)
    over(0, length, collect)
    for part in range(2):
        own_to_mate(0, part).wait_send()


def solution(mesh):
    row_size, col_size = mesh.shape["row"], mesh.shape["col"]
    length, chips = row_size // 2, col_size // 2
    dma = pltpu.SemaphoreType.DMA

    def local(tiles, stack_index, block_mask):
        stack, ids = tiles[0, 0], stack_index[0]
        slots, side, _ = stack.shape
        col_panel = pltpu.VMEM((col_size, slots, side, side), stack.dtype)
        purified = pl.pallas_call(
            functools.partial(kernel, row_size, col_size),
            out_shape=jax.ShapeDtypeStruct(stack.shape, stack.dtype),
            in_specs=[VMEM, SMEM, SMEM],
            out_specs=VMEM,
            scratch_shapes=[
                col_panel,
                pltpu.VMEM((row_size, slots, side, side), stack.dtype),
                col_panel,
                pltpu.VMEM(stack.shape, stack.dtype),
                pltpu.VMEM(stack.shape, jnp.float32),
                pltpu.VMEM((col_size, 8, 128), jnp.int32),
                pltpu.VMEM((row_size, 8, 128), jnp.int32),
                pltpu.VMEM((8, 128), jnp.int32),
                pltpu.SMEM((col_size, 8, 128), jnp.int32),
                pltpu.SMEM((row_size, 8, 128), jnp.int32),
                dma((4, chips, slots)),
                dma((8, chips, slots)),
                dma((4, 2, length, slots + 2)),
                dma((4, length, slots + 1)),
                dma((2, row_size)),
                dma((2, col_size)),
                dma((2,)),
            ],
            compiler_params=pltpu.CompilerParams(collective_id=0, has_side_effects=True),
            name="purify",
        )(stack, ids, block_mask)
        return purified[None, None]

    placed = (P("row", "col", None, None, None), P("row", "col", None), P())
    return jax.shard_map(
        local,
        mesh=mesh,
        in_specs=placed,
        out_specs=P("row", "col", None, None, None),
        check_vma=False,
    )
```

```python
import functools

import jax
import jax.numpy as jnp
from jax import lax
from jax.experimental import pallas as pl
from jax.experimental.pallas import tpu as pltpu
from jax.sharding import PartitionSpec as P

MESH = pl.DeviceIdType.MESH
VMEM = pl.BlockSpec(memory_space=pltpu.VMEM)
SMEM = pl.BlockSpec(memory_space=pltpu.SMEM)


def send(src, dst, send_sem, recv_sem, row, col):
    return pltpu.make_async_remote_copy(
        src_ref=src,
        dst_ref=dst,
        send_sem=send_sem,
        recv_sem=recv_sem,
        device_id=(row, col),
        device_id_type=MESH,
    )


def greet(row_size, col_size, row, col, with_rows):
    barrier = pltpu.get_barrier_semaphore()
    count = col_size - 1
    for step in range(1, col_size):
        peer = lax.rem(col + step, col_size)
        pl.semaphore_signal(barrier, inc=1, device_id=(row, peer), device_id_type=MESH)
    if with_rows:
        count += row_size - 1
        for step in range(1, row_size):
            peer = lax.rem(row + step, row_size)
            pl.semaphore_signal(barrier, inc=1, device_id=(peer, col), device_id_type=MESH)
    pl.semaphore_wait(barrier, count)


class ColGather:
    def __init__(self, row, col, col_size, slots, own, panel, sems):
        self.row, self.col, self.slots = row, col, slots
        self.own, self.panel, self.sems = own, panel, sems
        self.chips = col_size // 2
        self.chip, self.core = col // 2, lax.rem(col, 2)
        self.partner = col + 1 - 2 * self.core

    def across(self, step, slot):
        target = 2 * lax.rem(self.chip + step, self.chips) + self.core
        return send(
            self.own.at[slot], self.panel.at[self.col, slot],
            self.sems.at[0, step - 1, slot], self.sems.at[1, step - 1, slot], self.row, target,
        )

    def beside(self, step, slot):
        origin = 2 * lax.rem(self.chip + self.chips - step, self.chips) + self.core
        src = self.own.at[slot] if step == 0 else self.panel.at[origin, slot]
        return send(
            src, self.panel.at[origin, slot],
            self.sems.at[2, step, slot], self.sems.at[3, step, slot], self.row, self.partner,
        )

    def start(self):
        for slot in range(self.slots):
            for step in range(1, self.chips):
                self.across(step, slot).start()
        for slot in range(self.slots):
            self.beside(0, slot).start()

    def origin(self, step, core):
        return 2 * lax.rem(self.chip + self.chips - step, self.chips) + core

    def forward(self, use=None):
        for slot in range(self.slots):
            for step in range(1, self.chips):
                self.across(step, slot).wait_recv()
                self.beside(step, slot).start()
                if use is not None:
                    use(self.origin(step, self.core), slot)

    def collect(self, use, steps):
        for step in steps:
            for slot in range(self.slots):
                self.beside(step, slot).wait_recv()
                if use is not None:
                    use(self.origin(step, 1 - self.core), slot)

    def settle(self):
        for step in range(self.chips):
            for slot in range(self.slots):
                if step:
                    self.across(step, slot).wait_send()
                self.beside(step, slot).wait_send()


def kernel(
    row_size, col_size, tiles, ids, mask, out, left, right, squares, square, total, left_ids, right_ids, ids_out,
    left_labels, right_labels, col_sems, square_sems, line_sems, side_sems, row_id_sems, col_id_sems, label_sems,
):
    row, col = lax.axis_index("row"), lax.axis_index("col")
    slots, side = tiles.shape[0], tiles.shape[1]
    half = side // 2
    length = row_size // 2
    place, lane = row // 2, lax.rem(row, 2)
    mate = row + 1 - 2 * lane

    lane_iota = lax.broadcasted_iota(jnp.int32, (8, 128), 1)
    packed = jnp.full((8, 128), -1, jnp.int32)
    for slot in range(slots):
        packed = jnp.where(lane_iota == slot, ids[0, slot], packed)
    ids_out[...] = packed
    greet(row_size, col_size, row, col, True)

    pieces = [(slot, 0, side, False) for slot in range(slots - 1)]
    cut = side * 64 // 256
    pieces += [(slots - 1, cut, side - cut, False)]
    early = (slots - 1, 0, cut, True)
    mine = [early] + pieces
    count = len(mine)

    def view(ref, piece, origin=None):
        slot, first, rows, _ = piece
        if origin is None:
            return ref.at[slot, pl.ds(first, rows)]
        return ref.at[origin, slot, pl.ds(first, rows)]

    def to_mate(index, at):
        piece = mine[index]
        origin = 2 * at + lane
        return send(
            view(right, piece, origin), view(right, piece, origin),
            side_sems.at[0, at, index], side_sems.at[1, at, index], mate, col,
        )

    def own_to_mate(index):
        piece = mine[index]
        return send(
            view(tiles, piece), view(right, piece, row),
            side_sems.at[0, place, index], side_sems.at[1, place, index], mate, col,
        )

    def from_mate(index, at):
        piece = mine[index]
        origin = 2 * at + 1 - lane
        return send(
            view(right, piece, origin), view(right, piece, origin),
            side_sems.at[0, at, index], side_sems.at[1, at, index], mate, col,
        )

    def along(way, step, index, first=False):
        heading = 1 if way == 0 else -1
        piece = mine[0] if index == count else mine[index]
        on_lane = 1 - lane if index == count else lane
        origin = 2 * (place - heading * step) + on_lane
        src = view(tiles, piece) if first and index < count else view(right, piece, origin)
        return send(
            src, view(right, piece, origin),
            line_sems.at[way, 0, step, index], line_sems.at[way, 1, step, index],
            row + 2 * heading, col,
        )

    def landing(way, step, index):
        heading = 1 if way == 0 else -1
        piece = mine[0] if index == count else mine[index]
        on_lane = 1 - lane if index == count else lane
        origin = 2 * (place - heading * (step + 1)) + on_lane
        return send(
            view(right, piece, origin), view(right, piece, origin),
            line_sems.at[way, 0, step, index], line_sems.at[way, 1, step, index],
            row + 2 * heading, col,
        )

    can_send = (place + 1 < length, place > 0)

    def arrives(way, step):
        return place - step >= 1 if way == 0 else place + step + 1 < length

    def goes(way, step):
        if way == 0:
            return (place - step >= 0) & (place + 1 < length)
        return (place + step < length) & (place > 0)

    def id_row(step):
        return send(
            ids_out, right_ids.at[row], row_id_sems.at[0, step], row_id_sems.at[1, step],
            lax.rem(row + step, row_size), col,
        )

    def id_col(step):
        return send(
            ids_out, left_ids.at[col], col_id_sems.at[0, step], col_id_sems.at[1, step],
            row, lax.rem(col + step, col_size),
        )

    for step in range(1, row_size):
        id_row(step).start()
    for step in range(1, col_size):
        id_col(step).start()

    own_to_mate(0).start()
    for index in range(count):
        for way in range(2):
            @pl.when(can_send[way])
            def _():
                along(way, 0, index, True).start()
        if index:
            own_to_mate(index).start()
    left_gather = ColGather(row, col, col_size, slots, tiles, left, col_sems)
    left_gather.start()


    from_mate(0, place).wait_recv()
    for way in range(2):
        @pl.when(can_send[way])
        def _():
            along(way, 0, count).start()

    right[row] = tiles[...]
    left[col] = tiles[...]
    right_ids[row] = packed
    left_ids[col] = packed

    def turn(step, unused):
        for index in list(range(count)) + [count]:
            for way in range(2):
                @pl.when(arrives(way, step))
                def _():
                    landing(way, step, index).wait_recv()

                    @pl.when(can_send[way])
                    def _():
                        along(way, step + 1, index).start()

                    if 0 < index < count:
                        heading = 1 if way == 0 else -1
                        to_mate(index, place - heading * (step + 1)).start()
        return unused

    block_rows, block_cols = mask.shape[0] // row_size, mask.shape[1] // col_size
    owns = []
    for slot in range(slots):
        own = ids[0, slot]
        own_row, own_col = own // block_cols, lax.rem(own, block_cols)
        out_row, out_col = row * block_rows + own_row, col * block_cols + own_col
        owns.append((own_row, own_col, out_row, out_col, mask[out_row, out_col] > 0))

    def find(labels, region, wanted):
        spot, found = jnp.int32(0), labels[region, 0, 0] == wanted
        for other in range(1, slots):
            same = labels[region, 0, other] == wanted
            spot = jnp.where(same, other, spot)
            found = found | same
        return spot, found

    def square_term(origin, place):
        label = right_labels[origin, 0, place]
        inner = origin * block_rows + label // block_cols
        band = inner // block_cols
        chosen = []
        for own_row, own_col, out_row, out_col, live in owns:
            spot, found = find(left_labels, band, own_row * block_cols + lax.rem(inner, block_cols))
            use = live & found & (lax.rem(label, block_cols) == own_col)
            use = use & (mask[out_row, inner] > 0) & (mask[inner, out_col] > 0)
            tile = left[band, spot]
            chosen.append(jnp.where(use, tile, jnp.zeros_like(tile)))
        term = jnp.dot(
            jnp.concatenate(chosen, axis=0), right[origin, place], preferred_element_type=jnp.float32
        )
        total[...] += term.reshape(total.shape)

    def cube_term(origin, place):
        label = left_labels[origin, 0, place]
        inner = origin * block_cols + lax.rem(label, block_cols)
        band = inner // block_rows
        piece = squares[origin, place]
        for slot, (own_row, own_col, out_row, out_col, live) in enumerate(owns):
            spot, found = find(right_labels, band, lax.rem(inner, block_rows) * block_cols + own_col)
            use = live & found & (label // block_cols == own_row)
            use = use & (mask[out_row, inner] > 0) & (mask[inner, out_col] > 0)
            tile = right[band, spot]
            total[slot] += jnp.dot(
                piece, jnp.where(use, tile, jnp.zeros_like(tile)), preferred_element_type=jnp.float32
            )

    def stack_terms(origin, wait=None):
        for slot in range(slots):
            if wait is not None:
                wait(slot)
            square_term(origin, slot)

    def mate_terms(at):
        stack_terms(2 * at + 1 - lane, lambda slot: from_mate(slot + 1, at).wait_recv())

    def consume(step):
        for way in range(2):
            @pl.when(arrives(way, step))
            def _():
                heading = 1 if way == 0 else -1
                stack_terms(2 * (place - heading * (step + 1)) + lane)
        for way in range(2):
            @pl.when(arrives(way, step))
            def _():
                heading = 1 if way == 0 else -1
                mate_terms(place - heading * (step + 1))

    total[...] = jnp.zeros_like(total)
    turn(0, 0)
    for step in range(1, row_size):
        id_row(step).wait()
    for step in range(1, col_size):
        id_col(step).wait()
    copies = (
        pltpu.make_async_copy(left_ids, left_labels, label_sems.at[0]),
        pltpu.make_async_copy(right_ids, right_labels, label_sems.at[1]),
    )
    for copy in copies:
        copy.start()
    for copy in copies:
        copy.wait()
    left_gather.forward()
    left_gather.collect(None, range(left_gather.chips))
    stack_terms(row)
    mate_terms(place)

    def advance(step, unused):
        turn(step, 0)
        consume(step - 1)
        return unused

    lax.fori_loop(1, length - 1, advance, 0)
    consume(length - 2)

    square[...] = total[...].astype(square.dtype)

    def keep(slot, unused):
        squares[col, slot] = square[slot]
        return unused

    lax.fori_loop(0, slots, keep, 0)
    square_gather = ColGather(row, col, col_size, slots, square, squares, square_sems)
    square_gather.start()
    total[...] = jnp.zeros_like(total)
    for slot in range(slots):
        cube_term(col, slot)
    square_gather.collect(cube_term, [0])
    square_gather.forward(cube_term)
    square_gather.collect(cube_term, range(1, square_gather.chips))
    out[...] = (3.0 * square[...].astype(jnp.float32) - 2.0 * total[...]).astype(out.dtype)

    left_gather.settle()
    square_gather.settle()

    def settle(step, unused):
        for index in range(count + 1):
            for way in range(2):
                @pl.when(goes(way, step))
                def _():
                    along(way, step, index).wait_send()
        return unused

    lax.fori_loop(0, length - 1, settle, 0)
    own_to_mate(0).wait_send()

    def collect(at, unused):
        for index in range(1, count):
            to_mate(index, at).wait_send()
        return unused

    lax.fori_loop(0, length, collect, 0)


def solution(mesh):
    row_size, col_size = mesh.shape["row"], mesh.shape["col"]
    length, chips = row_size // 2, col_size // 2
    dma = pltpu.SemaphoreType.DMA

    def local(tiles, stack_index, block_mask):
        stack, ids = tiles[0, 0], stack_index[0]
        slots, side, _ = stack.shape
        col_panel = pltpu.VMEM((col_size, slots, side, side), stack.dtype)
        purified = pl.pallas_call(
            functools.partial(kernel, row_size, col_size),
            out_shape=jax.ShapeDtypeStruct(stack.shape, stack.dtype),
            in_specs=[VMEM, SMEM, SMEM],
            out_specs=VMEM,
            scratch_shapes=[
                col_panel,
                pltpu.VMEM((row_size, slots, side, side), stack.dtype),
                col_panel,
                pltpu.VMEM(stack.shape, stack.dtype),
                pltpu.VMEM(stack.shape, jnp.float32),
                pltpu.VMEM((col_size, 8, 128), jnp.int32),
                pltpu.VMEM((row_size, 8, 128), jnp.int32),
                pltpu.VMEM((8, 128), jnp.int32),
                pltpu.SMEM((col_size, 8, 128), jnp.int32),
                pltpu.SMEM((row_size, 8, 128), jnp.int32),
                dma((4, chips, slots)),
                dma((4, chips, slots)),
                dma((2, 2, length, slots + 2)),
                dma((2, length, slots + 1)),
                dma((2, row_size)),
                dma((2, col_size)),
                dma((2,)),
            ],
            compiler_params=pltpu.CompilerParams(collective_id=0, has_side_effects=True),
            name="purify",
        )(stack, ids, block_mask)
        return purified[None, None]

    placed = (P("row", "col", None, None, None), P("row", "col", None), P())
    return jax.shard_map(
        local,
        mesh=mesh,
        in_specs=placed,
        out_specs=P("row", "col", None, None, None),
        check_vma=False,
    )
```

```python
import functools

import jax
import jax.numpy as jnp
from jax import lax
from jax.experimental import pallas as pl
from jax.experimental.pallas import tpu as pltpu
from jax.sharding import PartitionSpec as P

MESH = pl.DeviceIdType.MESH
VMEM = pl.BlockSpec(memory_space=pltpu.VMEM)
SMEM = pl.BlockSpec(memory_space=pltpu.SMEM)


def send(src, dst, send_sem, recv_sem, row, col):
    return pltpu.make_async_remote_copy(
        src_ref=src,
        dst_ref=dst,
        send_sem=send_sem,
        recv_sem=recv_sem,
        device_id=(row, col),
        device_id_type=MESH,
    )


def greet(row_size, col_size, row, col, with_rows):
    barrier = pltpu.get_barrier_semaphore()
    count = col_size - 1
    for step in range(1, col_size):
        peer = lax.rem(col + step, col_size)
        pl.semaphore_signal(barrier, inc=1, device_id=(row, peer), device_id_type=MESH)
    if with_rows:
        count += row_size - 1
        for step in range(1, row_size):
            peer = lax.rem(row + step, row_size)
            pl.semaphore_signal(barrier, inc=1, device_id=(peer, col), device_id_type=MESH)
    pl.semaphore_wait(barrier, count)


class ColGather:
    def __init__(self, row, col, col_size, slots, own, panel, sems):
        self.row, self.col, self.slots = row, col, slots
        self.own, self.panel, self.sems = own, panel, sems
        self.chips = col_size // 2
        self.chip, self.core = col // 2, lax.rem(col, 2)
        self.partner = col + 1 - 2 * self.core

    def across(self, step, slot):
        target = 2 * lax.rem(self.chip + step, self.chips) + self.core
        return send(
            self.own.at[slot], self.panel.at[self.col, slot],
            self.sems.at[0, step - 1, slot], self.sems.at[1, step - 1, slot], self.row, target,
        )

    def beside(self, step, slot):
        origin = 2 * lax.rem(self.chip + self.chips - step, self.chips) + self.core
        src = self.own.at[slot] if step == 0 else self.panel.at[origin, slot]
        return send(
            src, self.panel.at[origin, slot],
            self.sems.at[2, step, slot], self.sems.at[3, step, slot], self.row, self.partner,
        )

    def start(self):
        for slot in range(self.slots):
            for step in range(1, self.chips):
                self.across(step, slot).start()
        for slot in range(self.slots):
            self.beside(0, slot).start()

    def origin(self, step, core):
        return 2 * lax.rem(self.chip + self.chips - step, self.chips) + core

    def forward(self, use=None):
        for slot in range(self.slots):
            for step in range(1, self.chips):
                self.across(step, slot).wait_recv()
                self.beside(step, slot).start()
                if use is not None:
                    use(self.origin(step, self.core), slot)

    def collect(self, use, steps):
        for step in steps:
            for slot in range(self.slots):
                self.beside(step, slot).wait_recv()
                if use is not None:
                    use(self.origin(step, 1 - self.core), slot)

    def settle(self):
        for step in range(self.chips):
            for slot in range(self.slots):
                if step:
                    self.across(step, slot).wait_send()
                self.beside(step, slot).wait_send()


def kernel(
    row_size, col_size, tiles, ids, mask, out, left, right, squares, square, total, left_ids, right_ids, ids_out,
    left_labels, right_labels, col_sems, square_sems, line_sems, side_sems, row_id_sems, col_id_sems, label_sems,
):
    row, col = lax.axis_index("row"), lax.axis_index("col")
    slots, side = tiles.shape[0], tiles.shape[1]
    half = side // 2
    length = row_size // 2
    place, lane = row // 2, lax.rem(row, 2)
    mate = row + 1 - 2 * lane

    lane_iota = lax.broadcasted_iota(jnp.int32, (8, 128), 1)
    packed = jnp.full((8, 128), -1, jnp.int32)
    for slot in range(slots):
        packed = jnp.where(lane_iota == slot, ids[0, slot], packed)
    ids_out[...] = packed
    greet(row_size, col_size, row, col, True)

    pieces = [(slot, 0, side, False) for slot in range(slots - 1)]
    cut = side * 64 // 256
    pieces += [(slots - 1, cut, side - cut, False)]
    early = (slots - 1, 0, cut, True)
    mine = [early] + pieces
    count = len(mine)

    def view(ref, piece, origin=None):
        slot, first, rows, _ = piece
        if origin is None:
            return ref.at[slot, pl.ds(first, rows)]
        return ref.at[origin, slot, pl.ds(first, rows)]

    def to_mate(index, at):
        piece = mine[index]
        origin = 2 * at + lane
        return send(
            view(right, piece, origin), view(right, piece, origin),
            side_sems.at[0, at, index], side_sems.at[1, at, index], mate, col,
        )

    def own_to_mate(index):
        piece = mine[index]
        return send(
            view(tiles, piece), view(right, piece, row),
            side_sems.at[0, place, index], side_sems.at[1, place, index], mate, col,
        )

    def from_mate(index, at):
        piece = mine[index]
        origin = 2 * at + 1 - lane
        return send(
            view(right, piece, origin), view(right, piece, origin),
            side_sems.at[0, at, index], side_sems.at[1, at, index], mate, col,
        )

    def along(way, step, index, first=False):
        heading = 1 if way == 0 else -1
        piece = mine[0] if index == count else mine[index]
        on_lane = 1 - lane if index == count else lane
        origin = 2 * (place - heading * step) + on_lane
        src = view(tiles, piece) if first and index < count else view(right, piece, origin)
        return send(
            src, view(right, piece, origin),
            line_sems.at[way, 0, step, index], line_sems.at[way, 1, step, index],
            row + 2 * heading, col,
        )

    def landing(way, step, index):
        heading = 1 if way == 0 else -1
        piece = mine[0] if index == count else mine[index]
        on_lane = 1 - lane if index == count else lane
        origin = 2 * (place - heading * (step + 1)) + on_lane
        return send(
            view(right, piece, origin), view(right, piece, origin),
            line_sems.at[way, 0, step, index], line_sems.at[way, 1, step, index],
            row + 2 * heading, col,
        )

    can_send = (place + 1 < length, place > 0)

    def arrives(way, step):
        return place - step >= 1 if way == 0 else place + step + 1 < length

    def goes(way, step):
        if way == 0:
            return (place - step >= 0) & (place + 1 < length)
        return (place + step < length) & (place > 0)

    def id_row(step):
        return send(
            ids_out, right_ids.at[row], row_id_sems.at[0, step], row_id_sems.at[1, step],
            lax.rem(row + step, row_size), col,
        )

    def id_col(step):
        return send(
            ids_out, left_ids.at[col], col_id_sems.at[0, step], col_id_sems.at[1, step],
            row, lax.rem(col + step, col_size),
        )

    for step in range(1, row_size):
        id_row(step).start()
    for step in range(1, col_size):
        id_col(step).start()

    left_gather = ColGather(row, col, col_size, slots, tiles, left, col_sems)
    left_gather.start()
    own_to_mate(0).start()
    for index in range(count):
        for way in range(2):
            @pl.when(can_send[way])
            def _():
                along(way, 0, index, True).start()
        if index:
            own_to_mate(index).start()


    from_mate(0, place).wait_recv()
    for way in range(2):
        @pl.when(can_send[way])
        def _():
            along(way, 0, count).start()

    right[row] = tiles[...]
    left[col] = tiles[...]
    right_ids[row] = packed
    left_ids[col] = packed

    def turn(step, unused):
        for index in list(range(count)) + [count]:
            for way in range(2):
                @pl.when(arrives(way, step))
                def _():
                    landing(way, step, index).wait_recv()

                    @pl.when(can_send[way])
                    def _():
                        along(way, step + 1, index).start()

                    if 0 < index < count:
                        heading = 1 if way == 0 else -1
                        to_mate(index, place - heading * (step + 1)).start()
        return unused

    block_rows, block_cols = mask.shape[0] // row_size, mask.shape[1] // col_size
    owns = []
    for slot in range(slots):
        own = ids[0, slot]
        own_row, own_col = own // block_cols, lax.rem(own, block_cols)
        out_row, out_col = row * block_rows + own_row, col * block_cols + own_col
        owns.append((own_row, own_col, out_row, out_col, mask[out_row, out_col] > 0))

    def find(labels, region, wanted):
        spot, found = jnp.int32(0), labels[region, 0, 0] == wanted
        for other in range(1, slots):
            same = labels[region, 0, other] == wanted
            spot = jnp.where(same, other, spot)
            found = found | same
        return spot, found

    def square_term(origin, place):
        label = right_labels[origin, 0, place]
        inner = origin * block_rows + label // block_cols
        band = inner // block_cols
        chosen = []
        for own_row, own_col, out_row, out_col, live in owns:
            spot, found = find(left_labels, band, own_row * block_cols + lax.rem(inner, block_cols))
            use = live & found & (lax.rem(label, block_cols) == own_col)
            use = use & (mask[out_row, inner] > 0) & (mask[inner, out_col] > 0)
            tile = left[band, spot]
            chosen.append(jnp.where(use, tile, jnp.zeros_like(tile)))
        term = jnp.dot(
            jnp.concatenate(chosen, axis=0), right[origin, place], preferred_element_type=jnp.float32
        )
        total[...] += term.reshape(total.shape)

    def cube_term(origin, place):
        label = left_labels[origin, 0, place]
        inner = origin * block_cols + lax.rem(label, block_cols)
        band = inner // block_rows
        piece = squares[origin, place]
        for slot, (own_row, own_col, out_row, out_col, live) in enumerate(owns):
            spot, found = find(right_labels, band, lax.rem(inner, block_rows) * block_cols + own_col)
            use = live & found & (label // block_cols == own_row)
            use = use & (mask[out_row, inner] > 0) & (mask[inner, out_col] > 0)
            tile = right[band, spot]
            total[slot] += jnp.dot(
                piece, jnp.where(use, tile, jnp.zeros_like(tile)), preferred_element_type=jnp.float32
            )

    def stack_terms(origin, wait=None):
        for slot in range(slots):
            if wait is not None:
                wait(slot)
            square_term(origin, slot)

    def mate_terms(at):
        stack_terms(2 * at + 1 - lane, lambda slot: from_mate(slot + 1, at).wait_recv())

    def consume(step):
        for way in range(2):
            @pl.when(arrives(way, step))
            def _():
                heading = 1 if way == 0 else -1
                stack_terms(2 * (place - heading * (step + 1)) + lane)
        for way in range(2):
            @pl.when(arrives(way, step))
            def _():
                heading = 1 if way == 0 else -1
                mate_terms(place - heading * (step + 1))

    total[...] = jnp.zeros_like(total)
    turn(0, 0)
    for step in range(1, row_size):
        id_row(step).wait()
    for step in range(1, col_size):
        id_col(step).wait()
    copies = (
        pltpu.make_async_copy(left_ids, left_labels, label_sems.at[0]),
        pltpu.make_async_copy(right_ids, right_labels, label_sems.at[1]),
    )
    for copy in copies:
        copy.start()
    for copy in copies:
        copy.wait()
    left_gather.forward()
    left_gather.collect(None, range(left_gather.chips))
    stack_terms(row)
    mate_terms(place)

    def advance(step, unused):
        turn(step, 0)
        consume(step - 1)
        return unused

    lax.fori_loop(1, length - 1, advance, 0)
    consume(length - 2)

    square[...] = total[...].astype(square.dtype)

    square_gather = ColGather(row, col, col_size, slots, square, squares, square_sems)

    def keep(slot, unused):
        squares[col, slot] = square[slot]
        for step in range(1, square_gather.chips):
            square_gather.across(step, slot).start()
        square_gather.beside(0, slot).start()
        return unused

    lax.fori_loop(0, slots, keep, 0)
    total[...] = jnp.zeros_like(total)
    for slot in range(slots):
        cube_term(col, slot)
    square_gather.collect(cube_term, [0])
    square_gather.forward(cube_term)
    square_gather.collect(cube_term, range(1, square_gather.chips))
    out[...] = (3.0 * square[...].astype(jnp.float32) - 2.0 * total[...]).astype(out.dtype)

    left_gather.settle()
    square_gather.settle()

    def settle(step, unused):
        for index in range(count + 1):
            for way in range(2):
                @pl.when(goes(way, step))
                def _():
                    along(way, step, index).wait_send()
        return unused

    lax.fori_loop(0, length - 1, settle, 0)
    own_to_mate(0).wait_send()

    def collect(at, unused):
        for index in range(1, count):
            to_mate(index, at).wait_send()
        return unused

    lax.fori_loop(0, length, collect, 0)


def solution(mesh):
    row_size, col_size = mesh.shape["row"], mesh.shape["col"]
    length, chips = row_size // 2, col_size // 2
    dma = pltpu.SemaphoreType.DMA

    def local(tiles, stack_index, block_mask):
        stack, ids = tiles[0, 0], stack_index[0]
        slots, side, _ = stack.shape
        col_panel = pltpu.VMEM((col_size, slots, side, side), stack.dtype)
        purified = pl.pallas_call(
            functools.partial(kernel, row_size, col_size),
            out_shape=jax.ShapeDtypeStruct(stack.shape, stack.dtype),
            in_specs=[VMEM, SMEM, SMEM],
            out_specs=VMEM,
            scratch_shapes=[
                col_panel,
                pltpu.VMEM((row_size, slots, side, side), stack.dtype),
                col_panel,
                pltpu.VMEM(stack.shape, stack.dtype),
                pltpu.VMEM(stack.shape, jnp.float32),
                pltpu.VMEM((col_size, 8, 128), jnp.int32),
                pltpu.VMEM((row_size, 8, 128), jnp.int32),
                pltpu.VMEM((8, 128), jnp.int32),
                pltpu.SMEM((col_size, 8, 128), jnp.int32),
                pltpu.SMEM((row_size, 8, 128), jnp.int32),
                dma((4, chips, slots)),
                dma((4, chips, slots)),
                dma((2, 2, length, slots + 2)),
                dma((2, length, slots + 1)),
                dma((2, row_size)),
                dma((2, col_size)),
                dma((2,)),
            ],
            compiler_params=pltpu.CompilerParams(collective_id=0, has_side_effects=True),
            name="purify",
        )(stack, ids, block_mask)
        return purified[None, None]

    placed = (P("row", "col", None, None, None), P("row", "col", None), P())
    return jax.shard_map(
        local,
        mesh=mesh,
        in_specs=placed,
        out_specs=P("row", "col", None, None, None),
        check_vma=False,
    )
```
